16 devices in a mesh: pool: 16 (over z, y, x, core).
Axes of the slice: x: 2, y: 2, z: 2, core: 2. Of those that a mesh axis runs over, the one named last changes fastest.
Arguments:
- queries: bfloat16 [64, 128, 40, 128], P('pool')
- k_new: bfloat16 [64, 128, 8, 128], P('pool')
- v_new: bfloat16 [64, 128, 8, 128], P('pool')
- k_pool: bfloat16 [8192, 16, 8, 128], P('pool')
- v_pool: bfloat16 [8192, 16, 8, 128], P('pool')
- block_table: int32 [64, 128], replicated
- write_ids: int32 [64, 8], P('pool')
Outputs:
- output 1: bfloat16 [64, 128, 40, 128], P('pool')
- output 2: bfloat16 [8192, 16, 8, 128], P('pool')
- output 3: bfloat16 [8192, 16, 8, 128], P('pool')
All inputs are finite; a program needn't handle non-finite values.
Results may differ from the reference program's by a relative error of at most 0.00950796.
Values are sent between devices in bfloat16 or wider.
A program may use at most 1 GiB of HBM per device.

```python
import jax
import jax.numpy as jnp
from jax import lax

NUM_DEVICES = 16
REQ_PER_DEV = 4
CHUNK_LEN = 128
PREFIX_BLOCKS = 128
BLOCKS_PER_DEV = 512
BLOCK_LEN = 16
Q_HEADS = 40
KV_HEADS = 8
HEAD_DIM = 128


def draw_tables(rng_key):
    key_first, key_choice, key_start, key_base, key_write = jax.random.split(rng_key, 5)
    quarter = BLOCKS_PER_DEV // 4
    half_len = PREFIX_BLOCKS // 2
    per_owner = 2 * PREFIX_BLOCKS // NUM_DEVICES
    first_dev = jax.random.randint(key_first, (), 0, NUM_DEVICES)
    dev_choice = jax.random.randint(key_choice, (NUM_DEVICES,), 0, 2)
    win_start = first_dev + jax.random.randint(key_start, (NUM_DEVICES,), 0, NUM_DEVICES // 4)
    row_base = jax.random.randint(key_base, (NUM_DEVICES, REQ_PER_DEV), 0, quarter)
    slot_idx = jnp.arange(half_len)
    pop_owner = (first_dev + slot_idx // per_owner) % NUM_DEVICES
    pop_local = dev_choice[:, None] * per_owner + slot_idx[None, :] % per_owner
    pop_ids = pop_owner[None, :] * BLOCKS_PER_DEV + pop_local
    pop_rows = jnp.broadcast_to(pop_ids[:, None, :], (NUM_DEVICES, REQ_PER_DEV, half_len))
    win_owner = (win_start[:, None] + slot_idx[None, :]) % NUM_DEVICES
    win_local = quarter + (row_base[:, :, None] + slot_idx[None, None, :] // NUM_DEVICES) % quarter
    win_rows = win_owner[:, None, :] * BLOCKS_PER_DEV + win_local
    block_tab = jnp.concatenate([pop_rows, win_rows], axis=-1)
    block_tab = block_tab.reshape(NUM_DEVICES * REQ_PER_DEV, PREFIX_BLOCKS)
    new_blocks = REQ_PER_DEV * CHUNK_LEN // BLOCK_LEN
    write_keys = jax.random.split(key_write, NUM_DEVICES)
    shuffled = jax.vmap(lambda one_key: jax.random.permutation(one_key, BLOCKS_PER_DEV // 2))(write_keys)
    write_tab = shuffled[:, :new_blocks] + BLOCKS_PER_DEV // 2
    write_tab = write_tab.reshape(NUM_DEVICES * REQ_PER_DEV, CHUNK_LEN // BLOCK_LEN)
    return block_tab.astype(jnp.int32), write_tab.astype(jnp.int32)


def setup_inputs(seed: int = 0) -> dict:
    key_q, key_kn, key_vn, key_kp, key_vp, key_tab = jax.random.split(jax.random.key(seed), 6)
    n_rows = NUM_DEVICES * REQ_PER_DEV
    chunk_kv = (n_rows, CHUNK_LEN, KV_HEADS, HEAD_DIM)
    pool_shape = (NUM_DEVICES * BLOCKS_PER_DEV, BLOCK_LEN, KV_HEADS, HEAD_DIM)
    queries = jax.random.normal(key_q, (n_rows, CHUNK_LEN, Q_HEADS, HEAD_DIM), jnp.float32)
    k_new = jax.random.normal(key_kn, chunk_kv, jnp.float32)
    v_new = jax.random.normal(key_vn, chunk_kv, jnp.float32)
    k_pool = jax.random.normal(key_kp, pool_shape, jnp.float32)
    v_pool = jax.random.normal(key_vp, pool_shape, jnp.float32)
    block_table, write_ids = draw_tables(key_tab)
    return {'queries': queries.astype(jnp.bfloat16), 'k_new': k_new.astype(jnp.bfloat16), 'v_new': v_new.astype(jnp.bfloat16), 'k_pool': k_pool.astype(jnp.bfloat16), 'v_pool': v_pool.astype(jnp.bfloat16), 'block_table': block_table, 'write_ids': write_ids}


def attend_one(q_rows, k_all, v_all):
    groups = Q_HEADS // KV_HEADS
    prefix_len = PREFIX_BLOCKS * BLOCK_LEN
    q_grp = q_rows.astype(jnp.float32).reshape(CHUNK_LEN, KV_HEADS, groups, HEAD_DIM)
    scores = jnp.einsum('cgqd,tgd->cgqt', q_grp, k_all.astype(jnp.float32)) * HEAD_DIM ** -0.5
    visible = jnp.arange(prefix_len + CHUNK_LEN)[None, :] <= prefix_len + jnp.arange(CHUNK_LEN)[:, None]
    scores = jnp.where(visible[:, None, None, :], scores, -jnp.inf)
    prob_rows = jax.nn.softmax(scores, axis=-1).astype(jnp.bfloat16).astype(jnp.float32)
    attn_rows = jnp.einsum('cgqt,tgd->cgqd', prob_rows, v_all.astype(jnp.float32))
    return attn_rows.reshape(CHUNK_LEN, Q_HEADS, HEAD_DIM).astype(jnp.bfloat16)


def reference(queries, k_new, v_new, k_pool, v_pool, block_table, write_ids):
    prefix_len = PREFIX_BLOCKS * BLOCK_LEN
    n_rows = NUM_DEVICES * REQ_PER_DEV

    def one_request(row_item):
        q_rows, k_chunk, v_chunk, row_ids = row_item
        k_all = jnp.concatenate([k_pool[row_ids].reshape(prefix_len, KV_HEADS, HEAD_DIM), k_chunk], axis=0)
        v_all = jnp.concatenate([v_pool[row_ids].reshape(prefix_len, KV_HEADS, HEAD_DIM), v_chunk], axis=0)
        return attend_one(q_rows, k_all, v_all)

    attn_out = lax.map(one_request, (queries, k_new, v_new, block_table))
    targets = ((jnp.arange(n_rows) // REQ_PER_DEV)[:, None] * BLOCKS_PER_DEV + write_ids).reshape(-1)
    new_shape = (n_rows * CHUNK_LEN // BLOCK_LEN, BLOCK_LEN, KV_HEADS, HEAD_DIM)
    k_pool_out = k_pool.at[targets].set(k_new.reshape(new_shape))
    v_pool_out = v_pool.at[targets].set(v_new.reshape(new_shape))
    return attn_out, k_pool_out, v_pool_out
```

```python
import functools

import jax
import jax.numpy as jnp
from jax import lax
from jax.experimental import pallas as pl
from jax.experimental.pallas import tpu as pltpu
from jax.sharding import PartitionSpec as P

FAST_CAP = 4
FULL_CAP = 20
RELAY_CAP = 2
SHARED_CAP = 8
GROUP = 8
STORE_BLOCKS = 16


def gather_kernel(ids_ref, k_hbm, v_hbm, out_ref, buf, sem):
    step, steps = pl.program_id(0), pl.num_programs(0)

    def fetch(at_step, slot):
        for i in range(GROUP):
            block = ids_ref[at_step * GROUP + i]
            pltpu.make_async_copy(k_hbm.at[block], buf.at[slot, i, 0], sem.at[slot]).start()
            pltpu.make_async_copy(v_hbm.at[block], buf.at[slot, i, 1], sem.at[slot]).start()

    @pl.when(step == 0)
    def _():
        fetch(0, 0)

    @pl.when(step + 1 < steps)
    def _():
        fetch(step + 1, (step + 1) % 2)

    slot = step % 2
    pltpu.make_async_copy(buf.at[slot], buf.at[slot], sem.at[slot]).wait()
    heads, block_len, dim = out_ref.shape[2:]
    rows = heads * block_len
    dst = lax.broadcasted_iota(jnp.int32, (rows, rows), 0)
    src = lax.broadcasted_iota(jnp.int32, (rows, rows), 1)
    perm = (src == (dst % block_len) * heads + dst // block_len).astype(jnp.bfloat16)
    for i in range(GROUP):
        pair = jnp.concatenate([buf[slot, i, 0], buf[slot, i, 1]], axis=1)
        moved = jnp.dot(perm, pair, preferred_element_type=jnp.float32).astype(jnp.bfloat16)
        out_ref[i, 0] = moved[:, :dim].reshape(heads, block_len, dim)
        out_ref[i, 1] = moved[:, dim:].reshape(heads, block_len, dim)


def gather_blocks(ids, k_flat, v_flat, heads, block_len):
    count, dim = ids.shape[0], k_flat.shape[-1]
    block = (GROUP, 2, heads, block_len, dim)
    return pl.pallas_call(
        gather_kernel,
        grid_spec=pltpu.PrefetchScalarGridSpec(
            num_scalar_prefetch=1,
            grid=(count // GROUP,),
            in_specs=[pl.BlockSpec(memory_space=pl.ANY)] * 2,
            out_specs=pl.BlockSpec(block, lambda i, ids: (i, 0, 0, 0, 0)),
            scratch_shapes=[
                pltpu.VMEM((2, GROUP, 2, heads * block_len, dim), jnp.bfloat16),
                pltpu.SemaphoreType.DMA((2,)),
            ],
        ),
        out_shape=jax.ShapeDtypeStruct((count,) + block[1:], jnp.bfloat16),
        cost_estimate=pl.CostEstimate(flops=count * 8 * 10 ** 6, bytes_accessed=count * 131072, transcendentals=0),
        name='gather_blocks',
    )(ids, k_flat, v_flat)


def store_kernel(from_ref, k_new_ref, v_new_ref, k_ref, v_ref, k_out, v_out):
    count = k_ref.shape[0]
    for i in range(count):
        new = from_ref[pl.program_id(0) * count + i]

        @pl.when(new < 0)
        def _():
            k_out[i] = k_ref[i]
            v_out[i] = v_ref[i]

        @pl.when(new >= 0)
        def _():
            k_out[i] = k_new_ref[new]
            v_out[i] = v_new_ref[new]


def store_chunk(write_ids, k_new, v_new, k_flat, v_flat):
    blocks, rows, dim = k_flat.shape
    k_new, v_new = k_new.reshape(-1, rows, dim), v_new.reshape(-1, rows, dim)
    targets = write_ids.reshape(-1)
    hit = targets[None, :] == jnp.arange(blocks)[:, None]
    from_new = jnp.sum(jnp.where(hit, jnp.arange(targets.shape[0]) + 1, 0), axis=1) - 1
    whole = pl.BlockSpec(k_new.shape, lambda i, ids: (0, 0, 0))
    part = pl.BlockSpec((STORE_BLOCKS, rows, dim), lambda i, ids: (i, 0, 0))
    return pl.pallas_call(
        store_kernel,
        grid_spec=pltpu.PrefetchScalarGridSpec(
            num_scalar_prefetch=1,
            grid=(blocks // STORE_BLOCKS,),
            in_specs=[whole, whole, part, part],
            out_specs=[part, part],
        ),
        out_shape=[jax.ShapeDtypeStruct(k_flat.shape, k_flat.dtype)] * 2,
        cost_estimate=pl.CostEstimate(flops=10 ** 10, bytes_accessed=8 * k_flat.size, transcendentals=0),
        name='store_chunk',
    )(from_new, k_new, v_new, k_flat, v_flat)


def attend_kernel(n_shared, code_ref, q_ref, kn_ref, vn_ref, shared_hbm, win_hbm, out_ref, k_buf, v_buf, sem):
    block_len = win_hbm.shape[3]
    n_pref = k_buf.shape[1] // block_len
    group, chunk, dim = out_ref.shape[2:]
    row_at = pl.program_id(0)
    head = pl.program_id(1)

    @pl.when(head == 0)
    def _():
        def fetch(e, carry):
            code = code_ref[row_at * n_pref + e]
            rows = pl.ds(pl.multiple_of(e * block_len, block_len), block_len)

            def pull(src, idx):
                pltpu.make_async_copy(src.at[idx, 0], k_buf.at[:, rows], sem.at[0]).start()
                pltpu.make_async_copy(src.at[idx, 1], v_buf.at[:, rows], sem.at[1]).start()

            if n_shared:
                @pl.when(code < n_shared)
                def _():
                    pull(shared_hbm, code)

                @pl.when(code >= n_shared)
                def _():
                    pull(win_hbm, code - n_shared)
            else:
                pull(win_hbm, code)
            return carry

        lax.fori_loop(0, n_pref, fetch, 0)
        pltpu.make_async_copy(k_buf, k_buf, sem.at[0]).wait()
        pltpu.make_async_copy(v_buf, v_buf, sem.at[1]).wait()

    keys, vals = k_buf[head], v_buf[head]
    k_self, v_self = kn_ref[0], vn_ref[0]
    contract = (((1,), (1,)), ((), ()))
    scale = dim ** -0.5
    row = lax.broadcasted_iota(jnp.int32, (chunk, chunk), 0)
    col = lax.broadcasted_iota(jnp.int32, (chunk, chunk), 1)
    for i in range(group):
        q = q_ref[0, pl.ds(i * chunk, chunk)]
        s_pref = lax.dot_general(q, keys, contract, preferred_element_type=jnp.float32) * scale
        s_self = lax.dot_general(q, k_self, contract, preferred_element_type=jnp.float32) * scale
        s_self = jnp.where(col <= row, s_self, -jnp.inf)
        top = jnp.maximum(jnp.max(s_pref, axis=1, keepdims=True), jnp.max(s_self, axis=1, keepdims=True))
        e_pref, e_self = jnp.exp(s_pref - top), jnp.exp(s_self - top)
        total = jnp.sum(e_pref, axis=1, keepdims=True) + jnp.sum(e_self, axis=1, keepdims=True)
        inv = 1.0 / total
        out = jnp.dot((e_pref * inv).astype(jnp.bfloat16), vals, preferred_element_type=jnp.float32)
        out += jnp.dot((e_self * inv).astype(jnp.bfloat16), v_self, preferred_element_type=jnp.float32)
        out_ref[0, 0, i] = out.astype(jnp.bfloat16)


def attend_rows(r, count, codes, q_t, kn_t, vn_t, shared, window):
    heads, rows, dim = q_t.shape[1:]
    chunk = kn_t.shape[2]
    block_len, n_pref = window.shape[3], codes.shape[1]
    group = rows // chunk
    n_shared = 0 if shared is None else shared.shape[0]
    operands = (window, window) if shared is None else (shared, window)
    row_spec = lambda n: pl.BlockSpec((None, 1, n, dim), lambda i, h, c: (r + i, h, 0, 0))
    keys = n_pref * block_len + chunk
    return pl.pallas_call(
        functools.partial(attend_kernel, n_shared),
        grid_spec=pltpu.PrefetchScalarGridSpec(
            num_scalar_prefetch=1,
            grid=(count, heads),
            in_specs=[row_spec(rows), row_spec(chunk), row_spec(chunk)] + [pl.BlockSpec(memory_space=pl.ANY)] * 2,
            out_specs=pl.BlockSpec((1, 1, group, chunk, dim), lambda i, h, c: (i, h, 0, 0, 0)),
            scratch_shapes=[
                pltpu.VMEM((heads, n_pref * block_len, dim), jnp.bfloat16),
                pltpu.VMEM((heads, n_pref * block_len, dim), jnp.bfloat16),
                pltpu.SemaphoreType.DMA((2,)),
            ],
        ),
        out_shape=jax.ShapeDtypeStruct((count, heads, group, chunk, dim), jnp.bfloat16),
        compiler_params=pltpu.CompilerParams(vmem_limit_bytes=48 * 2 ** 20),
        cost_estimate=pl.CostEstimate(
            flops=8 * count * heads * rows * keys * dim, bytes_accessed=count * 12 * 2 ** 20,
            transcendentals=count * heads * rows * keys),
        name='attend_rows',
    )(codes[r:r + count].reshape(-1), q_t, kn_t, vn_t, *operands)


def tri(n, strict=True):
    a, b = jnp.arange(n)[:, None], jnp.arange(n)[None, :]
    return (a < b if strict else a <= b).astype(jnp.float32)


def solution(mesh):
    n_dev = mesh.shape['pool']

    def local_step(queries, k_new, v_new, k_pool, v_pool, block_table, write_ids):
        req_count, chunk_len, q_heads, head_dim = queries.shape
        kv_heads = k_new.shape[2]
        per_dev, block_len = k_pool.shape[:2]
        n_pref = block_table.shape[1]
        groups = q_heads // kv_heads
        me = lax.axis_index('pool')

        tab = block_table.reshape(n_dev, req_count, n_pref)
        owners = block_table // per_dev
        local_ids = block_table % per_dev
        first = tab[:, 0]
        in_all = (first[:, None, :, None] == tab[:, 1:, None, :]).any(-1).all(1)
        shared = ((tab[..., None] == first[:, None, None, :]) & in_all[:, None, None, :]).any(-1)
        shared = shared.reshape(n_dev * req_count, n_pref)

        lanes = 128
        n_hi = n_dev * per_dev // lanes
        flat_first, flat_in = first.reshape(-1), in_all.reshape(-1)
        hot_hi = ((flat_first // lanes)[:, None] == jnp.arange(n_hi)) & flat_in[:, None]
        hot_lo = (flat_first % lanes)[:, None] == jnp.arange(lanes)
        named = jnp.einsum('eh,el->hl', hot_hi.astype(jnp.bfloat16), hot_lo.astype(jnp.bfloat16),
                           preferred_element_type=jnp.float32) > 0
        named_f = named.astype(jnp.float32)
        before = named_f @ tri(lanes)
        hi_count = jnp.sum(named_f, axis=1)
        hi_before = hi_count @ tri(n_hi)
        rank = (before + hi_before[:, None]).astype(jnp.int32)
        owner_count = jnp.sum(hi_count.reshape(n_dev, -1), axis=1).astype(jnp.int32)
        owner_base = hi_before[::n_hi // n_dev].astype(jnp.int32)

        win_count = jnp.sum((owners[:, :, None] == jnp.arange(n_dev)) & ~shared[:, :, None], axis=1)
        fits = (jnp.max(win_count) <= FAST_CAP) & (jnp.max(owner_count) <= RELAY_CAP * n_dev)
        fits = fits & (jnp.sum(owner_count) <= SHARED_CAP * n_dev)

        k_flat = k_pool.reshape(per_dev, block_len * kv_heads, head_dim)
        v_flat = v_pool.reshape(per_dev, block_len * kv_heads, head_dim)
        gather = lambda ids: gather_blocks(ids, k_flat, v_flat, kv_heads, block_len)
        exchange = lambda x: lax.all_to_all(x, 'pool', 0, 0, tiled=True)

        def slots(is_window, cap):
            mine = (owners == me) & is_window
            place = (mine.astype(jnp.float32) @ tri(n_pref)).astype(jnp.int32)
            pick = mine[:, None, :] & (place[:, None, :] == jnp.arange(cap)[:, None])
            send = jnp.sum(jnp.where(pick, local_ids[:, None, :], 0), axis=2)
            rows = lambda x: lax.dynamic_slice_in_dim(x, me * req_count, req_count, 0)
            own, win = rows(owners), rows(is_window)
            earlier = (own[:, :, None] == own[:, None, :]) & win[:, None, :] & (tri(n_pref).T > 0)
            code = own * cap + jnp.sum(earlier, axis=2)
            return send.reshape(n_dev, req_count, cap), code

        def prepare():
            q_t = queries.reshape(req_count, chunk_len, kv_heads, groups, head_dim).transpose(0, 2, 3, 1, 4)
            q_t = q_t.reshape(req_count, kv_heads, groups * chunk_len, head_dim)
            stored = store_chunk(write_ids, k_new, v_new, k_flat, v_flat)
            return (q_t, k_new.transpose(0, 2, 1, 3), v_new.transpose(0, 2, 1, 3)), stored

        def unpack(rows):
            rows = rows.reshape(-1, q_heads, chunk_len, head_dim)
            return rows.transpose(0, 2, 1, 3)

        def fast():
            my_base = lax.dynamic_index_in_dim(owner_base, me, keepdims=False)
            j = jnp.arange(n_dev)[:, None]
            want = my_base + jnp.arange(RELAY_CAP) * n_dev + (j - my_base) % n_dev
            mine = per_dev // lanes
            my_named = lax.dynamic_slice_in_dim(named, me * mine, mine, 0).reshape(-1)
            my_rank = lax.dynamic_slice_in_dim(rank, me * mine, mine, 0).reshape(-1)
            pick = my_named & (my_rank == want.reshape(-1)[:, None])
            relay_ids = jnp.sum(jnp.where(pick, jnp.arange(per_dev), 0), axis=1)
            relayed = exchange(gather(relay_ids))

            t_rank = jnp.arange(SHARED_CAP) * n_dev + me
            owner_end = owner_base + owner_count
            t_owner = jnp.minimum(jnp.sum(owner_end[None, :] <= t_rank[:, None], axis=1), n_dev - 1)
            t_base = jnp.sum(jnp.where(t_owner[:, None] == jnp.arange(n_dev), owner_base, 0), axis=1)
            t_slot = jnp.clip((t_rank - t_base) // n_dev, 0, RELAY_CAP - 1)
            shared_blocks = lax.all_gather(relayed[t_owner * RELAY_CAP + t_slot], 'pool', axis=0, tiled=True)

            send, code = slots(~shared, FAST_CAP)
            my_tab = lax.dynamic_slice_in_dim(block_table, me * req_count, req_count, 0).reshape(-1)
            my_hi = ((my_tab // lanes)[:, None] == jnp.arange(n_hi)).astype(jnp.float32)
            my_lo = (my_tab % lanes)[:, None] == jnp.arange(lanes)
            my_rank_of = jnp.sum(jnp.where(my_lo, my_hi @ jnp.minimum(rank, 255).astype(jnp.float32), 0), axis=1)
            my_rank_of = my_rank_of.astype(jnp.int32).reshape(req_count, n_pref)
            shared_code = (my_rank_of % n_dev) * SHARED_CAP + my_rank_of // n_dev
            my_shared = lax.dynamic_slice_in_dim(shared, me * req_count, req_count, 0)
            codes = jnp.where(my_shared, shared_code, n_dev * SHARED_CAP + code)

            done, rows, gate = [], [], None
            for r in range(req_count):
                blocks = gather(send[:, r].reshape(-1))
                if r == 1:
                    chunk, stored = prepare()
                    blocks, chunk, stored = lax.optimization_barrier((blocks, chunk, stored))
                if r >= 2:
                    rows.append(attend_rows(r - 2, 1, codes, *chunk, shared_blocks, done[r - 2]))
                    blocks, rows[-1] = lax.optimization_barrier((blocks, rows[-1]))
                done.append(exchange(blocks))
            for r in range(req_count - 2, req_count):
                rows.append(attend_rows(r, 1, codes, *chunk, shared_blocks, done[r]))
            return jnp.concatenate([unpack(x) for x in rows]), *stored

        def full():
            send, codes = slots(jnp.ones_like(shared), FULL_CAP)
            blocks = exchange(gather(send.reshape(-1)))
            places = codes // FULL_CAP * (req_count * FULL_CAP) + codes % FULL_CAP
            places += jnp.arange(req_count)[:, None] * FULL_CAP
            chunk, stored = prepare()
            return unpack(attend_rows(0, req_count, places, *chunk, None, blocks)), *stored

        attn, k_out, v_out = lax.cond(fits, fast, full)
        return attn, k_out.reshape(k_pool.shape), v_out.reshape(v_pool.shape)

    row_spec = P('pool')
    return jax.shard_map(local_step, mesh=mesh, in_specs=(row_spec, row_spec, row_spec, row_spec, row_spec, P(), row_spec), out_specs=(row_spec, row_spec, row_spec), check_vma=False)
```

```python
import functools

import jax
import jax.numpy as jnp
from jax import lax
from jax.experimental import pallas as pl
from jax.experimental.pallas import tpu as pltpu
from jax.sharding import PartitionSpec as P

FAST_CAP = 4
FULL_CAP = 20
RELAY_CAP = 2
SHARED_CAP = 8
GROUP = 8
STORE_BLOCKS = 16
GROUP_HEADS = 5
PAIR = 2
CORES = 2
N_CHIPS = 8
EARLY = 3
TILE = 1024
BUF_KEYS = 2048
LIST_PAD = 8
LOG2E = 1.4426950408889634


def gather_kernel(ids_ref, k_hbm, v_hbm, out_ref, buf, sem):
    step, steps = pl.program_id(0), pl.num_programs(0)

    def fetch(at_step, slot):
        for i in range(GROUP):
            block = ids_ref[at_step * GROUP + i]
            pltpu.make_async_copy(k_hbm.at[block], buf.at[slot, i, 0], sem.at[slot]).start()
            pltpu.make_async_copy(v_hbm.at[block], buf.at[slot, i, 1], sem.at[slot]).start()

    @pl.when(step == 0)
    def _():
        fetch(0, 0)

    @pl.when(step + 1 < steps)
    def _():
        fetch(step + 1, (step + 1) % 2)

    slot = step % 2
    pltpu.make_async_copy(buf.at[slot], buf.at[slot], sem.at[slot]).wait()
    heads, block_len, dim = out_ref.shape[2:]
    rows = heads * block_len
    dst = lax.broadcasted_iota(jnp.int32, (rows, rows), 0)
    src = lax.broadcasted_iota(jnp.int32, (rows, rows), 1)
    perm = (src == (dst % block_len) * heads + dst // block_len).astype(jnp.bfloat16)
    for i in range(GROUP):
        pair = jnp.concatenate([buf[slot, i, 0], buf[slot, i, 1]], axis=1)
        moved = jnp.dot(perm, pair, preferred_element_type=jnp.float32).astype(jnp.bfloat16)
        out_ref[i, 0] = moved[:, :dim].reshape(heads, block_len, dim)
        out_ref[i, 1] = moved[:, dim:].reshape(heads, block_len, dim)


def gather_blocks(ids, k_flat, v_flat, heads, block_len):
    count, dim = ids.shape[0], k_flat.shape[-1]
    block = (GROUP, 2, heads, block_len, dim)
    return pl.pallas_call(
        gather_kernel,
        grid_spec=pltpu.PrefetchScalarGridSpec(
            num_scalar_prefetch=1,
            grid=(count // GROUP,),
            in_specs=[pl.BlockSpec(memory_space=pl.ANY)] * 2,
            out_specs=pl.BlockSpec(block, lambda i, ids: (i, 0, 0, 0, 0)),
            scratch_shapes=[
                pltpu.VMEM((2, GROUP, 2, heads * block_len, dim), jnp.bfloat16),
                pltpu.SemaphoreType.DMA((2,)),
            ],
        ),
        out_shape=jax.ShapeDtypeStruct((count,) + block[1:], jnp.bfloat16),
        cost_estimate=pl.CostEstimate(flops=count * 8 * 10 ** 6, bytes_accessed=count * 131072, transcendentals=0),
        name='gather_blocks',
    )(ids, k_flat, v_flat)


def store_kernel(from_ref, k_new_ref, v_new_ref, k_ref, v_ref, k_out, v_out):
    count = k_ref.shape[0]
    for i in range(count):
        new = from_ref[pl.program_id(0) * count + i]

        @pl.when(new < 0)
        def _():
            k_out[i] = k_ref[i]
            v_out[i] = v_ref[i]

        @pl.when(new >= 0)
        def _():
            k_out[i] = k_new_ref[new]
            v_out[i] = v_new_ref[new]


def store_chunk(write_ids, k_new, v_new, k_flat, v_flat):
    blocks, rows, dim = k_flat.shape
    k_new, v_new = k_new.reshape(-1, rows, dim), v_new.reshape(-1, rows, dim)
    targets = write_ids.reshape(-1)
    hit = targets[None, :] == jnp.arange(blocks)[:, None]
    from_new = jnp.sum(jnp.where(hit, jnp.arange(targets.shape[0]) + 1, 0), axis=1) - 1
    whole = pl.BlockSpec(k_new.shape, lambda i, ids: (0, 0, 0))
    part = pl.BlockSpec((STORE_BLOCKS, rows, dim), lambda i, ids: (i, 0, 0))
    return pl.pallas_call(
        store_kernel,
        grid_spec=pltpu.PrefetchScalarGridSpec(
            num_scalar_prefetch=1,
            grid=(blocks // STORE_BLOCKS,),
            in_specs=[whole, whole, part, part],
            out_specs=[part, part],
        ),
        out_shape=[jax.ShapeDtypeStruct(k_flat.shape, k_flat.dtype)] * 2,
        cost_estimate=pl.CostEstimate(flops=10 ** 10, bytes_accessed=8 * k_flat.size, transcendentals=0),
        name='store_chunk',
    )(from_new, k_new, v_new, k_flat, v_flat)


def fetch_list(count, at, codes_ref, src_hbm, k_buf, v_buf, sem):
    block_len = src_hbm.shape[3]

    def fetch(e, carry):
        code = codes_ref[at + e]
        rows = pl.ds(pl.multiple_of(e * block_len, block_len), block_len)
        pltpu.make_async_copy(src_hbm.at[code, 0], k_buf.at[:, rows], sem.at[0]).start()
        pltpu.make_async_copy(src_hbm.at[code, 1], v_buf.at[:, rows], sem.at[1]).start()
        return carry

    def settle(t, carry):
        rows = pl.ds(0, TILE)
        pltpu.make_async_copy(k_buf.at[:, rows], k_buf.at[:, rows], sem.at[0]).wait()
        pltpu.make_async_copy(v_buf.at[:, rows], v_buf.at[:, rows], sem.at[1]).wait()
        return carry

    tiles = pl.cdiv(count * block_len, TILE)
    lax.fori_loop(0, tiles * (TILE // block_len), fetch, 0)
    lax.fori_loop(0, tiles, settle, 0)


def scores(q, keys):
    return lax.dot_general(q, keys, (((1,), (1,)), ((), ())), preferred_element_type=jnp.float32)


def wide_row(x, n):
    return jnp.concatenate([x] * (n // x.shape[1]), axis=1)


def scan_tiles(pair, keys, factor, q, k_buf, v_buf, top_ref, sum_ref, acc_ref):
    def body(t, carry):
        rows = pl.ds(pl.multiple_of(t * TILE, TILE), TILE)
        col = lax.broadcasted_iota(jnp.int32, (1, TILE), 1)
        bias = jnp.where(col < keys - t * TILE, 0.0, -jnp.inf)
        for j in range(PAIR):
            head = pair * PAIR + j
            s = scores(q[j], k_buf[head, rows]) + bias
            old = top_ref[j]
            top = jnp.maximum(old, jnp.max(s, axis=1, keepdims=True))
            shrink = jnp.exp2((old - top) * factor)
            p = jnp.exp2(s * factor - wide_row(top * factor, TILE))
            sum_ref[j] = sum_ref[j] * shrink + jnp.sum(p, axis=1, keepdims=True)
            part = jnp.dot(p.astype(jnp.bfloat16), v_buf[head, rows], preferred_element_type=jnp.float32)
            acc_ref[j] = acc_ref[j] * shrink + part
            top_ref[j] = top
        return carry

    lax.fori_loop(0, pl.cdiv(keys, TILE), body, 0)


def shared_kernel(codes_ref, q_ref, kn_ref, vn_ref, src_hbm, acc_ref, stat_ref, k_buf, v_buf, top_ref, sum_ref, sem):
    count = codes_ref[0]
    pair = pl.program_id(0)

    @pl.when((pair == 0) & (pl.program_id(1) == 0))
    def _():
        fetch_list(count, 1, codes_ref, src_hbm, k_buf, v_buf, sem)

    _, rows, dim = q_ref.shape
    chunk = kn_ref.shape[1]
    factor = dim ** -0.5 * LOG2E
    row = lax.broadcasted_iota(jnp.int32, (rows, chunk), 0) % chunk
    col = lax.broadcasted_iota(jnp.int32, (rows, chunk), 1)
    for j in range(PAIR):
        s = jnp.where(col <= row, scores(q_ref[j], kn_ref[j]), -jnp.inf)
        top = jnp.max(s, axis=1, keepdims=True)
        p = jnp.exp2(s * factor - top * factor)
        top_ref[j] = jnp.broadcast_to(top, (rows, dim))
        sum_ref[j] = jnp.broadcast_to(jnp.sum(p, axis=1, keepdims=True), (rows, dim))
        acc_ref[j] = jnp.dot(p.astype(jnp.bfloat16), vn_ref[j], preferred_element_type=jnp.float32)
    scan_tiles(pair, count * src_hbm.shape[3], factor, q_ref, k_buf, v_buf, top_ref, sum_ref, acc_ref)
    lane = lax.broadcasted_iota(jnp.int32, (rows, dim), 1)
    for j in range(PAIR):
        stat_ref[j] = jnp.where(lane == 0, top_ref[j], sum_ref[j])


def window_kernel(codes_ref, q_ref, acc_in, stat_in, src_hbm, old_ref, out_ref, k_buf, v_buf, top_ref, sum_ref, acc_ref, wide, sem):
    at = pl.program_id(0) * codes_ref.shape[0] // pl.num_programs(0)
    count = codes_ref[at]
    pair = pl.program_id(1)

    @pl.when(pair == 0)
    def _():
        fetch_list(count, at + 1, codes_ref, src_hbm, k_buf, v_buf, sem)

    _, rows, dim = q_ref.shape
    heads = k_buf.shape[0]
    chunk = rows // GROUP_HEADS
    for j in range(PAIR):
        top_ref[j] = jnp.broadcast_to(stat_in[j, :, 0:1], (rows, dim))
        sum_ref[j] = jnp.broadcast_to(stat_in[j, :, 1:2], (rows, dim))
        acc_ref[j] = acc_in[j]
    factor = dim ** -0.5 * LOG2E
    scan_tiles(pair, count * src_hbm.shape[3], factor, q_ref, k_buf, v_buf, top_ref, sum_ref, acc_ref)
    for j in range(PAIR):
        out = acc_ref[j] * (1.0 / sum_ref[j])
        for i in range(GROUP_HEADS):
            at_head = (pair * PAIR + j) * GROUP_HEADS + i
            wide[pl.ds(at_head, chunk, stride=heads * GROUP_HEADS), :] = out[i * chunk:(i + 1) * chunk]

    @pl.when(pair == heads // PAIR - 1)
    def _():
        out_ref[...] = wide[...].astype(jnp.bfloat16)


def attend_shared(codes, q_t, kn_t, vn_t, source):
    count, heads, rows, dim = q_t.shape
    chunk = kn_t.shape[2]
    part = lambda n: pl.BlockSpec((None, PAIR, n, dim), lambda h, i, c: (i, h, 0, 0))
    buf = pltpu.VMEM((heads, BUF_KEYS, dim), jnp.bfloat16)
    stat = pltpu.VMEM((PAIR, rows, dim), jnp.float32)
    state = jax.ShapeDtypeStruct(q_t.shape, jnp.float32)
    return pl.pallas_call(
        shared_kernel,
        grid_spec=pltpu.PrefetchScalarGridSpec(
            num_scalar_prefetch=1,
            grid=(heads // PAIR, count),
            in_specs=[part(rows), part(chunk), part(chunk), pl.BlockSpec(memory_space=pl.ANY)],
            out_specs=[part(rows), part(rows)],
            scratch_shapes=[buf, buf, stat, stat, pltpu.SemaphoreType.DMA((2,))],
        ),
        out_shape=[state, state],
        compiler_params=pltpu.CompilerParams(vmem_limit_bytes=48 * 2 ** 20),
        cost_estimate=pl.CostEstimate(
            flops=6 * q_t.size * 1152, bytes_accessed=40 * 2 ** 20, transcendentals=q_t.size * 9),
        name='attend_shared',
    )(codes, q_t, kn_t, vn_t, source)


def attend_window(first, count, codes, q_t, acc, stats, source, old):
    total, heads, rows, dim = q_t.shape
    part = pl.BlockSpec((None, PAIR, rows, dim), lambda i, h, c: (first + i, h, 0, 0))
    anywhere = pl.BlockSpec(memory_space=pl.ANY)
    buf = pltpu.VMEM((heads, BUF_KEYS, dim), jnp.bfloat16)
    stat = pltpu.VMEM((PAIR, rows, dim), jnp.float32)
    specs, operands, alias = [part, part, part, anywhere], [q_t, acc, stats, source], {}
    body = window_kernel
    if old is None:
        inner = body
        body = lambda c, q, a, s, src, *rest: inner(c, q, a, s, src, None, *rest)
    else:
        specs, operands, alias = specs + [anywhere], operands + [old], {5: 0}
    return pl.pallas_call(
        body,
        grid_spec=pltpu.PrefetchScalarGridSpec(
            num_scalar_prefetch=1,
            grid=(count, heads // PAIR),
            in_specs=specs,
            out_specs=pl.BlockSpec((None, heads * rows, dim), lambda i, h, c: (first + i, 0, 0)),
            scratch_shapes=[buf, buf, stat, stat, pltpu.VMEM((PAIR, rows, dim), jnp.float32),
                            pltpu.VMEM((heads * rows, dim), jnp.float32), pltpu.SemaphoreType.DMA((2,))],
        ),
        out_shape=jax.ShapeDtypeStruct((total, heads * rows, dim), jnp.bfloat16),
        input_output_aliases=alias,
        compiler_params=pltpu.CompilerParams(vmem_limit_bytes=48 * 2 ** 20),
        cost_estimate=pl.CostEstimate(
            flops=6 * count * heads * rows * dim * 1024, bytes_accessed=count * 12 * 2 ** 20,
            transcendentals=count * heads * rows * 1024),
        name='attend_window',
    )(codes.reshape(-1), *operands)


def listing(codes, keep):
    keep_i = keep.astype(jnp.int32)
    n = codes.shape[1]
    place = jnp.sum(jnp.where(jnp.arange(n)[:, None] > jnp.arange(n), keep_i[:, None, :], 0), axis=2)
    pick = keep[:, None, :] & (place[:, None, :] == jnp.arange(n + LIST_PAD - 1)[:, None])
    packed = jnp.sum(jnp.where(pick, codes[:, None, :], 0), axis=2)
    return jnp.concatenate([jnp.sum(keep_i, axis=1, keepdims=True), packed], axis=1)


def spread(blocks, n_dev):
    chips = n_dev // CORES
    groups = [list(range(core, n_dev, CORES)) for core in range(CORES)]
    copies = jnp.broadcast_to(blocks[None], (chips,) + blocks.shape).reshape((-1,) + blocks.shape[1:])
    got = lax.all_to_all(copies, 'pool', 0, 0, axis_index_groups=groups, tiled=True)
    return got, lax.ppermute(got, 'pool', [(i, i ^ 1) for i in range(n_dev)])


def spread_place(device, slot, me):
    chips_first = (device // CORES) * SHARED_CAP + slot
    return chips_first + jnp.where(device % CORES == me % CORES, 0, N_CHIPS * SHARED_CAP)


def tri(n, strict=True):
    a, b = jnp.arange(n)[:, None], jnp.arange(n)[None, :]
    return (a < b if strict else a <= b).astype(jnp.float32)


def solution(mesh):
    n_dev = mesh.shape['pool']

    def local_step(queries, k_new, v_new, k_pool, v_pool, block_table, write_ids):
        req_count, chunk_len, q_heads, head_dim = queries.shape
        kv_heads = k_new.shape[2]
        per_dev, block_len = k_pool.shape[:2]
        n_pref = block_table.shape[1]
        groups = q_heads // kv_heads
        me = lax.axis_index('pool')

        tab = block_table.reshape(n_dev, req_count, n_pref)
        owners = block_table // per_dev
        local_ids = block_table % per_dev
        first = tab[:, 0]
        in_all = (first[:, None, :, None] == tab[:, 1:, None, :]).any(-1).all(1)
        shared = ((tab[..., None] == first[:, None, None, :]) & in_all[:, None, None, :]).any(-1)
        shared = shared.reshape(n_dev * req_count, n_pref)

        lanes = 128
        n_hi = n_dev * per_dev // lanes
        flat_first, flat_in = first.reshape(-1), in_all.reshape(-1)
        hot_hi = ((flat_first // lanes)[:, None] == jnp.arange(n_hi)) & flat_in[:, None]
        hot_lo = (flat_first % lanes)[:, None] == jnp.arange(lanes)
        named = jnp.einsum('eh,el->hl', hot_hi.astype(jnp.bfloat16), hot_lo.astype(jnp.bfloat16),
                           preferred_element_type=jnp.float32) > 0
        named_f = named.astype(jnp.float32)
        before = named_f @ tri(lanes)
        hi_count = jnp.sum(named_f, axis=1)
        hi_before = hi_count @ tri(n_hi)
        rank = (before + hi_before[:, None]).astype(jnp.int32)
        owner_count = jnp.sum(hi_count.reshape(n_dev, -1), axis=1).astype(jnp.int32)
        owner_base = hi_before[::n_hi // n_dev].astype(jnp.int32)

        win_count = jnp.sum((owners[:, :, None] == jnp.arange(n_dev)) & ~shared[:, :, None], axis=1)
        fits = (jnp.max(win_count) <= FAST_CAP) & (jnp.max(owner_count) <= RELAY_CAP * n_dev)
        fits = fits & (jnp.sum(owner_count) <= SHARED_CAP * n_dev)

        k_flat = k_pool.reshape(per_dev, block_len * kv_heads, head_dim)
        v_flat = v_pool.reshape(per_dev, block_len * kv_heads, head_dim)
        gather = lambda ids: gather_blocks(ids, k_flat, v_flat, kv_heads, block_len)
        exchange = lambda x: lax.all_to_all(x, 'pool', 0, 0, tiled=True)

        def slots(is_window, cap):
            mine = (owners == me) & is_window
            place = (mine.astype(jnp.float32) @ tri(n_pref)).astype(jnp.int32)
            pick = mine[:, None, :] & (place[:, None, :] == jnp.arange(cap)[:, None])
            send = jnp.sum(jnp.where(pick, local_ids[:, None, :], 0), axis=2)
            rows = lambda x: lax.dynamic_slice_in_dim(x, me * req_count, req_count, 0)
            own, win = rows(owners), rows(is_window)
            earlier = (own[:, :, None] == own[:, None, :]) & win[:, None, :] & (tri(n_pref).T > 0)
            code = own * cap + jnp.sum(earlier, axis=2)
            return send.reshape(n_dev, req_count, cap), code

        def prepare():
            q_t = queries.reshape(req_count, chunk_len, kv_heads, groups, head_dim).transpose(0, 2, 3, 1, 4)
            q_t = q_t.reshape(req_count, kv_heads, groups * chunk_len, head_dim)
            stored = store_chunk(write_ids, k_new, v_new, k_flat, v_flat)
            return (q_t, k_new.transpose(0, 2, 1, 3), v_new.transpose(0, 2, 1, 3)), stored

        my_base = lax.dynamic_index_in_dim(owner_base, me, keepdims=False)
        j = jnp.arange(n_dev)[:, None]
        want = my_base + jnp.arange(RELAY_CAP) * n_dev + (j - my_base) % n_dev
        mine = per_dev // lanes
        my_named = lax.dynamic_slice_in_dim(named, me * mine, mine, 0).reshape(-1)
        my_rank = lax.dynamic_slice_in_dim(rank, me * mine, mine, 0).reshape(-1)
        pick = my_named & (my_rank == want.reshape(-1)[:, None])
        relay_ids = jnp.sum(jnp.where(pick, jnp.arange(per_dev), 0), axis=1)
        relayed = exchange(gather(relay_ids))
        send, code = slots(~shared, FAST_CAP)
        early = gather(send[:, :EARLY].reshape(-1))
        relayed, early = lax.optimization_barrier((relayed, early))

        def fast():
            t_rank = jnp.arange(SHARED_CAP) * n_dev + me
            owner_end = owner_base + owner_count
            t_owner = jnp.minimum(jnp.sum(owner_end[None, :] <= t_rank[:, None], axis=1), n_dev - 1)
            t_base = jnp.sum(jnp.where(t_owner[:, None] == jnp.arange(n_dev), owner_base, 0), axis=1)
            t_slot = jnp.clip((t_rank - t_base) // n_dev, 0, RELAY_CAP - 1)
            near, far = spread(relayed[t_owner * RELAY_CAP + t_slot], n_dev)
            chunk, stored = prepare()
            late = gather(send[:, EARLY:].reshape(-1))
            ready, near, chunk, late = lax.optimization_barrier((early, near, chunk, late))
            shared_blocks = jnp.concatenate([near, far])
            my_shared = lax.dynamic_slice_in_dim(shared, me * req_count, req_count, 0)
            my_tab = lax.dynamic_slice_in_dim(block_table, me * req_count, 1, 0).reshape(-1)
            my_hi = ((my_tab // lanes)[:, None] == jnp.arange(n_hi)).astype(jnp.float32)
            my_lo = (my_tab % lanes)[:, None] == jnp.arange(lanes)
            my_rank_of = jnp.sum(jnp.where(my_lo, my_hi @ jnp.minimum(rank, 255).astype(jnp.float32), 0), axis=1)
            my_rank_of = my_rank_of.astype(jnp.int32)
            shared_code = spread_place(my_rank_of % n_dev, my_rank_of // n_dev, me)
            shared_list = listing(shared_code[None], my_shared[:1])
            own, slot = code // FAST_CAP, code % FAST_CAP
            place = lambda r, n: own[r] * (n * FAST_CAP) + slot[r]
            early_code = jnp.stack([place(r, EARLY) + r * FAST_CAP for r in range(EARLY)])
            n_late = req_count - EARLY
            late_code = jnp.stack([place(EARLY + r, n_late) + r * FAST_CAP for r in range(n_late)])
            early_list, late_list = listing(early_code, ~my_shared[:EARLY]), listing(late_code, ~my_shared[EARLY:])

            early_win = exchange(ready)
            acc, stats = attend_shared(shared_list.reshape(-1), *chunk, shared_blocks)
            late, acc, stats, stored = lax.optimization_barrier((late, acc, stats, stored))
            late_win = exchange(late)
            attn = attend_window(0, EARLY, early_list, chunk[0], acc, stats, early_win, None)
            attn = attend_window(EARLY, n_late, late_list, chunk[0], acc, stats, late_win, attn)
            return attn, *stored

        def full():
            send, codes = slots(jnp.ones_like(shared), FULL_CAP)
            blocks = exchange(gather(send.reshape(-1)))
            places = codes // FULL_CAP * (req_count * FULL_CAP) + codes % FULL_CAP
            places += jnp.arange(req_count)[:, None] * FULL_CAP
            chunk, stored = prepare()
            none = jnp.zeros((n_pref + LIST_PAD,), jnp.int32)
            acc, stats = attend_shared(none, *chunk, blocks)
            lists = listing(places, jnp.ones_like(places, dtype=bool))
            return attend_window(0, req_count, lists, chunk[0], acc, stats, blocks, None), *stored

        attn, k_out, v_out = lax.cond(fits, fast, full)
        return attn.reshape(queries.shape), k_out.reshape(k_pool.shape), v_out.reshape(v_pool.shape)

    row_spec = P('pool')
    return jax.shard_map(local_step, mesh=mesh, in_specs=(row_spec, row_spec, row_spec, row_spec, row_spec, P(), row_spec), out_specs=(row_spec, row_spec, row_spec), check_vma=False)
```

```python
import functools

import jax
import jax.numpy as jnp
from jax import lax
from jax.experimental import pallas as pl
from jax.experimental.pallas import tpu as pltpu
from jax.sharding import PartitionSpec as P

FAST_CAP = 4
FULL_CAP = 20
RELAY_CAP = 2
SHARED_CAP = 8
GROUP = 16
STORE_BLOCKS = 16
GROUP_HEADS = 5
PAIR = 2
CORES = 2
N_CHIPS = 8
EARLY = 3
TILE = 1024
BUF_KEYS = 2048
LIST_PAD = 8
LOG2E = 1.4426950408889634


def gather_kernel(ids_ref, k_hbm, v_hbm, out_ref, buf, sem):
    step, steps = pl.program_id(0), pl.num_programs(0)

    def fetch(at_step, slot):
        for i in range(GROUP):
            block = ids_ref[at_step * GROUP + i]
            pltpu.make_async_copy(k_hbm.at[block], buf.at[slot, i, 0], sem.at[slot]).start()
            pltpu.make_async_copy(v_hbm.at[block], buf.at[slot, i, 1], sem.at[slot]).start()

    @pl.when(step == 0)
    def _():
        fetch(0, 0)

    @pl.when(step + 1 < steps)
    def _():
        fetch(step + 1, (step + 1) % 2)

    slot = step % 2
    pltpu.make_async_copy(buf.at[slot], buf.at[slot], sem.at[slot]).wait()
    heads, block_len, dim = out_ref.shape[2:]
    rows = heads * block_len
    dst = lax.broadcasted_iota(jnp.int32, (rows, rows), 0)
    src = lax.broadcasted_iota(jnp.int32, (rows, rows), 1)
    perm = (src == (dst % block_len) * heads + dst // block_len).astype(jnp.bfloat16)
    for i in range(GROUP):
        pair = jnp.concatenate([buf[slot, i, 0], buf[slot, i, 1]], axis=1)
        moved = jnp.dot(perm, pair, preferred_element_type=jnp.float32).astype(jnp.bfloat16)
        out_ref[i, 0] = moved[:, :dim].reshape(heads, block_len, dim)
        out_ref[i, 1] = moved[:, dim:].reshape(heads, block_len, dim)


def gather_blocks(ids, k_flat, v_flat, heads, block_len):
    count, dim = ids.shape[0], k_flat.shape[-1]
    block = (GROUP, 2, heads, block_len, dim)
    return pl.pallas_call(
        gather_kernel,
        grid_spec=pltpu.PrefetchScalarGridSpec(
            num_scalar_prefetch=1,
            grid=(count // GROUP,),
            in_specs=[pl.BlockSpec(memory_space=pl.ANY)] * 2,
            out_specs=pl.BlockSpec(block, lambda i, ids: (i, 0, 0, 0, 0)),
            scratch_shapes=[
                pltpu.VMEM((2, GROUP, 2, heads * block_len, dim), jnp.bfloat16),
                pltpu.SemaphoreType.DMA((2,)),
            ],
        ),
        out_shape=jax.ShapeDtypeStruct((count,) + block[1:], jnp.bfloat16),
        cost_estimate=pl.CostEstimate(flops=count * 8 * 10 ** 6, bytes_accessed=count * 131072, transcendentals=0),
        name='gather_blocks',
    )(ids, k_flat, v_flat)


def store_kernel(from_ref, k_new_ref, v_new_ref, k_ref, v_ref, k_out, v_out):
    count = k_ref.shape[0]
    for i in range(count):
        new = from_ref[pl.program_id(0) * count + i]

        @pl.when(new < 0)
        def _():
            k_out[i] = k_ref[i]
            v_out[i] = v_ref[i]

        @pl.when(new >= 0)
        def _():
            k_out[i] = k_new_ref[new]
            v_out[i] = v_new_ref[new]


def store_chunk(write_ids, k_new, v_new, k_flat, v_flat):
    blocks, rows, dim = k_flat.shape
    k_new, v_new = k_new.reshape(-1, rows, dim), v_new.reshape(-1, rows, dim)
    targets = write_ids.reshape(-1)
    hit = targets[None, :] == jnp.arange(blocks)[:, None]
    from_new = jnp.sum(jnp.where(hit, jnp.arange(targets.shape[0]) + 1, 0), axis=1) - 1
    whole = pl.BlockSpec(k_new.shape, lambda i, ids: (0, 0, 0))
    part = pl.BlockSpec((STORE_BLOCKS, rows, dim), lambda i, ids: (i, 0, 0))
    return pl.pallas_call(
        store_kernel,
        grid_spec=pltpu.PrefetchScalarGridSpec(
            num_scalar_prefetch=1,
            grid=(blocks // STORE_BLOCKS,),
            in_specs=[whole, whole, part, part],
            out_specs=[part, part],
        ),
        out_shape=[jax.ShapeDtypeStruct(k_flat.shape, k_flat.dtype)] * 2,
        cost_estimate=pl.CostEstimate(flops=10 ** 10, bytes_accessed=8 * k_flat.size, transcendentals=0),
        name='store_chunk',
    )(from_new, k_new, v_new, k_flat, v_flat)


def fetch_list(count, at, codes_ref, src_hbm, k_buf, v_buf, sem):
    block_len = src_hbm.shape[3]

    def fetch(e, carry):
        code = codes_ref[at + e]
        rows = pl.ds(pl.multiple_of(e * block_len, block_len), block_len)
        pltpu.make_async_copy(src_hbm.at[code, 0], k_buf.at[:, rows], sem.at[0]).start()
        pltpu.make_async_copy(src_hbm.at[code, 1], v_buf.at[:, rows], sem.at[1]).start()
        return carry

    def settle(t, carry):
        rows = pl.ds(0, TILE)
        pltpu.make_async_copy(k_buf.at[:, rows], k_buf.at[:, rows], sem.at[0]).wait()
        pltpu.make_async_copy(v_buf.at[:, rows], v_buf.at[:, rows], sem.at[1]).wait()
        return carry

    tiles = pl.cdiv(count * block_len, TILE)
    lax.fori_loop(0, tiles * (TILE // block_len), fetch, 0)
    lax.fori_loop(0, tiles, settle, 0)


def scores(q, keys):
    return lax.dot_general(q, keys, (((1,), (1,)), ((), ())), preferred_element_type=jnp.float32)


def wide_row(x, n):
    return jnp.concatenate([x] * (n // x.shape[1]), axis=1)


def scan_tiles(pair, keys, factor, q, k_buf, v_buf, top_ref, sum_ref, acc_ref):
    def body(t, carry):
        rows = pl.ds(pl.multiple_of(t * TILE, TILE), TILE)
        col = lax.broadcasted_iota(jnp.int32, (1, TILE), 1)
        bias = jnp.where(col < keys - t * TILE, 0.0, -jnp.inf)
        for j in range(PAIR):
            head = pair * PAIR + j
            s = scores(q[j], k_buf[head, rows]) + bias
            old = top_ref[j]
            top = jnp.maximum(old, jnp.max(s, axis=1, keepdims=True))
            shrink = jnp.exp2((old - top) * factor)
            p = jnp.exp2(s * factor - wide_row(top * factor, TILE))
            sum_ref[j] = sum_ref[j] * shrink + jnp.sum(p, axis=1, keepdims=True)
            part = jnp.dot(p.astype(jnp.bfloat16), v_buf[head, rows], preferred_element_type=jnp.float32)
            acc_ref[j] = acc_ref[j] * shrink + part
            top_ref[j] = top
        return carry

    lax.fori_loop(0, pl.cdiv(keys, TILE), body, 0)


def shared_kernel(codes_ref, q_ref, kn_ref, vn_ref, src_hbm, acc_ref, stat_ref, k_buf, v_buf, top_ref, sum_ref, sem):
    count = codes_ref[0]
    pair = pl.program_id(0)

    @pl.when((pair == 0) & (pl.program_id(1) == 0))
    def _():
        fetch_list(count, 1, codes_ref, src_hbm, k_buf, v_buf, sem)

    _, rows, dim = q_ref.shape
    chunk = kn_ref.shape[1]
    factor = dim ** -0.5 * LOG2E
    row = lax.broadcasted_iota(jnp.int32, (rows, chunk), 0) % chunk
    col = lax.broadcasted_iota(jnp.int32, (rows, chunk), 1)
    for j in range(PAIR):
        s = jnp.where(col <= row, scores(q_ref[j], kn_ref[j]), -jnp.inf)
        top = jnp.max(s, axis=1, keepdims=True)
        p = jnp.exp2(s * factor - top * factor)
        top_ref[j] = jnp.broadcast_to(top, (rows, dim))
        sum_ref[j] = jnp.broadcast_to(jnp.sum(p, axis=1, keepdims=True), (rows, dim))
        acc_ref[j] = jnp.dot(p.astype(jnp.bfloat16), vn_ref[j], preferred_element_type=jnp.float32)
    scan_tiles(pair, count * src_hbm.shape[3], factor, q_ref, k_buf, v_buf, top_ref, sum_ref, acc_ref)
    lane = lax.broadcasted_iota(jnp.int32, (rows, dim), 1)
    for j in range(PAIR):
        stat_ref[j] = jnp.where(lane == 0, top_ref[j], sum_ref[j])


def window_kernel(codes_ref, q_ref, acc_in, stat_in, src_hbm, old_ref, out_ref, k_buf, v_buf, top_ref, sum_ref, acc_ref, wide, sem):
    at = pl.program_id(0) * codes_ref.shape[0] // pl.num_programs(0)
    count = codes_ref[at]
    pair = pl.program_id(1)

    @pl.when(pair == 0)
    def _():
        fetch_list(count, at + 1, codes_ref, src_hbm, k_buf, v_buf, sem)

    _, rows, dim = q_ref.shape
    heads = k_buf.shape[0]
    chunk = rows // GROUP_HEADS
    for j in range(PAIR):
        top_ref[j] = jnp.broadcast_to(stat_in[j, :, 0:1], (rows, dim))
        sum_ref[j] = jnp.broadcast_to(stat_in[j, :, 1:2], (rows, dim))
        acc_ref[j] = acc_in[j]
    factor = dim ** -0.5 * LOG2E
    scan_tiles(pair, count * src_hbm.shape[3], factor, q_ref, k_buf, v_buf, top_ref, sum_ref, acc_ref)
    for j in range(PAIR):
        out = acc_ref[j] * (1.0 / sum_ref[j])
        for i in range(GROUP_HEADS):
            at_head = (pair * PAIR + j) * GROUP_HEADS + i
            wide[pl.ds(at_head, chunk, stride=heads * GROUP_HEADS), :] = out[i * chunk:(i + 1) * chunk]

    @pl.when(pair == heads // PAIR - 1)
    def _():
        out_ref[...] = wide[...].astype(jnp.bfloat16)


def attend_shared(codes, q_t, kn_t, vn_t, source):
    count, heads, rows, dim = q_t.shape
    chunk = kn_t.shape[2]
    part = lambda n: pl.BlockSpec((None, PAIR, n, dim), lambda h, i, c: (i, h, 0, 0))
    buf = pltpu.VMEM((heads, BUF_KEYS, dim), jnp.bfloat16)
    stat = pltpu.VMEM((PAIR, rows, dim), jnp.float32)
    state = jax.ShapeDtypeStruct(q_t.shape, jnp.float32)
    return pl.pallas_call(
        shared_kernel,
        grid_spec=pltpu.PrefetchScalarGridSpec(
            num_scalar_prefetch=1,
            grid=(heads // PAIR, count),
            in_specs=[part(rows), part(chunk), part(chunk), pl.BlockSpec(memory_space=pl.ANY)],
            out_specs=[part(rows), part(rows)],
            scratch_shapes=[buf, buf, stat, stat, pltpu.SemaphoreType.DMA((2,))],
        ),
        out_shape=[state, state],
        compiler_params=pltpu.CompilerParams(vmem_limit_bytes=48 * 2 ** 20),
        cost_estimate=pl.CostEstimate(
            flops=6 * q_t.size * 1152, bytes_accessed=40 * 2 ** 20, transcendentals=q_t.size * 9),
        name='attend_shared',
    )(codes, q_t, kn_t, vn_t, source)


def attend_window(first, count, codes, q_t, acc, stats, source, old):
    total, heads, rows, dim = q_t.shape
    part = pl.BlockSpec((None, PAIR, rows, dim), lambda i, h, c: (first + i, h, 0, 0))
    anywhere = pl.BlockSpec(memory_space=pl.ANY)
    buf = pltpu.VMEM((heads, BUF_KEYS, dim), jnp.bfloat16)
    stat = pltpu.VMEM((PAIR, rows, dim), jnp.float32)
    specs, operands, alias = [part, part, part, anywhere], [q_t, acc, stats, source], {}
    body = window_kernel
    if old is None:
        inner = body
        body = lambda c, q, a, s, src, *rest: inner(c, q, a, s, src, None, *rest)
    else:
        specs, operands, alias = specs + [anywhere], operands + [old], {5: 0}
    return pl.pallas_call(
        body,
        grid_spec=pltpu.PrefetchScalarGridSpec(
            num_scalar_prefetch=1,
            grid=(count, heads // PAIR),
            in_specs=specs,
            out_specs=pl.BlockSpec((None, heads * rows, dim), lambda i, h, c: (first + i, 0, 0)),
            scratch_shapes=[buf, buf, stat, stat, pltpu.VMEM((PAIR, rows, dim), jnp.float32),
                            pltpu.VMEM((heads * rows, dim), jnp.float32), pltpu.SemaphoreType.DMA((2,))],
        ),
        out_shape=jax.ShapeDtypeStruct((total, heads * rows, dim), jnp.bfloat16),
        input_output_aliases=alias,
        compiler_params=pltpu.CompilerParams(vmem_limit_bytes=48 * 2 ** 20),
        cost_estimate=pl.CostEstimate(
            flops=6 * count * heads * rows * dim * 1024, bytes_accessed=count * 12 * 2 ** 20,
            transcendentals=count * heads * rows * 1024),
        name='attend_window',
    )(codes.reshape(-1), *operands)


def listing(codes, keep):
    keep_i = keep.astype(jnp.int32)
    n = codes.shape[1]
    place = jnp.sum(jnp.where(jnp.arange(n)[:, None] > jnp.arange(n), keep_i[:, None, :], 0), axis=2)
    pick = keep[:, None, :] & (place[:, None, :] == jnp.arange(n + LIST_PAD - 1)[:, None])
    packed = jnp.sum(jnp.where(pick, codes[:, None, :], 0), axis=2)
    return jnp.concatenate([jnp.sum(keep_i, axis=1, keepdims=True), packed], axis=1)


def spread(blocks, n_dev):
    chips = n_dev // CORES
    groups = [list(range(core, n_dev, CORES)) for core in range(CORES)]
    copies = jnp.broadcast_to(blocks[None], (chips,) + blocks.shape).reshape((-1,) + blocks.shape[1:])
    got = lax.all_to_all(copies, 'pool', 0, 0, axis_index_groups=groups, tiled=True)
    return got, lax.ppermute(got, 'pool', [(i, i ^ 1) for i in range(n_dev)])


def spread_place(device, slot, me):
    chips_first = (device // CORES) * SHARED_CAP + slot
    return chips_first + jnp.where(device % CORES == me % CORES, 0, N_CHIPS * SHARED_CAP)


def tri(n, strict=True):
    a, b = jnp.arange(n)[:, None], jnp.arange(n)[None, :]
    return (a < b if strict else a <= b).astype(jnp.float32)


def solution(mesh):
    n_dev = mesh.shape['pool']

    def local_step(queries, k_new, v_new, k_pool, v_pool, block_table, write_ids):
        req_count, chunk_len, q_heads, head_dim = queries.shape
        kv_heads = k_new.shape[2]
        per_dev, block_len = k_pool.shape[:2]
        n_pref = block_table.shape[1]
        groups = q_heads // kv_heads
        me = lax.axis_index('pool')

        tab = block_table.reshape(n_dev, req_count, n_pref)
        owners = block_table // per_dev
        local_ids = block_table % per_dev
        first = tab[:, 0]
        in_all = (first[:, None, :, None] == tab[:, 1:, None, :]).any(-1).all(1)
        shared = ((tab[..., None] == first[:, None, None, :]) & in_all[:, None, None, :]).any(-1)
        shared = shared.reshape(n_dev * req_count, n_pref)

        lanes = 128
        n_hi = n_dev * per_dev // lanes
        flat_first, flat_in = first.reshape(-1), in_all.reshape(-1)
        hot_hi = ((flat_first // lanes)[:, None] == jnp.arange(n_hi)) & flat_in[:, None]
        hot_lo = (flat_first % lanes)[:, None] == jnp.arange(lanes)
        named = jnp.einsum('eh,el->hl', hot_hi.astype(jnp.bfloat16), hot_lo.astype(jnp.bfloat16),
                           preferred_element_type=jnp.float32) > 0
        named_f = named.astype(jnp.float32)
        before = named_f @ tri(lanes)
        hi_count = jnp.sum(named_f, axis=1)
        hi_before = hi_count @ tri(n_hi)
        rank = (before + hi_before[:, None]).astype(jnp.int32)
        owner_count = jnp.sum(hi_count.reshape(n_dev, -1), axis=1).astype(jnp.int32)
        owner_base = hi_before[::n_hi // n_dev].astype(jnp.int32)

        win_count = jnp.sum((owners[:, :, None] == jnp.arange(n_dev)) & ~shared[:, :, None], axis=1)
        fits = (jnp.max(win_count) <= FAST_CAP) & (jnp.max(owner_count) <= RELAY_CAP * n_dev)
        fits = fits & (jnp.sum(owner_count) <= SHARED_CAP * n_dev)

        k_flat = k_pool.reshape(per_dev, block_len * kv_heads, head_dim)
        v_flat = v_pool.reshape(per_dev, block_len * kv_heads, head_dim)
        gather = lambda ids: gather_blocks(ids, k_flat, v_flat, kv_heads, block_len)
        exchange = lambda x: lax.all_to_all(x, 'pool', 0, 0, tiled=True)

        def slots(is_window, cap):
            mine = (owners == me) & is_window
            place = (mine.astype(jnp.float32) @ tri(n_pref)).astype(jnp.int32)
            pick = mine[:, None, :] & (place[:, None, :] == jnp.arange(cap)[:, None])
            send = jnp.sum(jnp.where(pick, local_ids[:, None, :], 0), axis=2)
            rows = lambda x: lax.dynamic_slice_in_dim(x, me * req_count, req_count, 0)
            own, win = rows(owners), rows(is_window)
            earlier = (own[:, :, None] == own[:, None, :]) & win[:, None, :] & (tri(n_pref).T > 0)
            code = own * cap + jnp.sum(earlier, axis=2)
            return send.reshape(n_dev, req_count, cap), code

        def prepare():
            q_t = queries.reshape(req_count, chunk_len, kv_heads, groups, head_dim).transpose(0, 2, 3, 1, 4)
            q_t = q_t.reshape(req_count, kv_heads, groups * chunk_len, head_dim)
            stored = store_chunk(write_ids, k_new, v_new, k_flat, v_flat)
            return (q_t, k_new.transpose(0, 2, 1, 3), v_new.transpose(0, 2, 1, 3)), stored

        my_base = lax.dynamic_index_in_dim(owner_base, me, keepdims=False)
        j = jnp.arange(n_dev)[:, None]
        want = my_base + jnp.arange(RELAY_CAP) * n_dev + (j - my_base) % n_dev
        mine = per_dev // lanes
        my_named = lax.dynamic_slice_in_dim(named, me * mine, mine, 0).reshape(-1)
        my_rank = lax.dynamic_slice_in_dim(rank, me * mine, mine, 0).reshape(-1)
        pick = my_named & (my_rank == want.reshape(-1)[:, None])
        relay_ids = jnp.sum(jnp.where(pick, jnp.arange(per_dev), 0), axis=1)
        relayed = exchange(gather(relay_ids))
        send, code = slots(~shared, FAST_CAP)
        early = gather(send[:, :EARLY].reshape(-1))
        relayed, early = lax.optimization_barrier((relayed, early))

        def fast():
            t_rank = jnp.arange(SHARED_CAP) * n_dev + me
            owner_end = owner_base + owner_count
            t_owner = jnp.minimum(jnp.sum(owner_end[None, :] <= t_rank[:, None], axis=1), n_dev - 1)
            t_base = jnp.sum(jnp.where(t_owner[:, None] == jnp.arange(n_dev), owner_base, 0), axis=1)
            t_slot = jnp.clip((t_rank - t_base) // n_dev, 0, RELAY_CAP - 1)
            near, far = spread(relayed[t_owner * RELAY_CAP + t_slot], n_dev)
            chunk, stored = prepare()
            late = gather(send[:, EARLY:].reshape(-1))
            ready, near, chunk, late = lax.optimization_barrier((early, near, chunk, late))
            shared_blocks = jnp.concatenate([near, far])
            my_shared = lax.dynamic_slice_in_dim(shared, me * req_count, req_count, 0)
            my_tab = lax.dynamic_slice_in_dim(block_table, me * req_count, 1, 0).reshape(-1)
            my_hi = ((my_tab // lanes)[:, None] == jnp.arange(n_hi)).astype(jnp.float32)
            my_lo = (my_tab % lanes)[:, None] == jnp.arange(lanes)
            my_rank_of = jnp.sum(jnp.where(my_lo, my_hi @ jnp.minimum(rank, 255).astype(jnp.float32), 0), axis=1)
            my_rank_of = my_rank_of.astype(jnp.int32)
            shared_code = spread_place(my_rank_of % n_dev, my_rank_of // n_dev, me)
            shared_list = listing(shared_code[None], my_shared[:1])
            own, slot = code // FAST_CAP, code % FAST_CAP
            place = lambda r, n: own[r] * (n * FAST_CAP) + slot[r]
            early_code = jnp.stack([place(r, EARLY) + r * FAST_CAP for r in range(EARLY)])
            n_late = req_count - EARLY
            late_code = jnp.stack([place(EARLY + r, n_late) + r * FAST_CAP for r in range(n_late)])
            early_list, late_list = listing(early_code, ~my_shared[:EARLY]), listing(late_code, ~my_shared[EARLY:])

            early_win = exchange(ready)
            acc, stats = attend_shared(shared_list.reshape(-1), *chunk, shared_blocks)
            late, acc, stats, stored = lax.optimization_barrier((late, acc, stats, stored))
            late_win = exchange(late)
            attn = attend_window(0, EARLY, early_list, chunk[0], acc, stats, early_win, None)
            attn = attend_window(EARLY, n_late, late_list, chunk[0], acc, stats, late_win, attn)
            return attn, *stored

        def full():
            send, codes = slots(jnp.ones_like(shared), FULL_CAP)
            blocks = exchange(gather(send.reshape(-1)))
            places = codes // FULL_CAP * (req_count * FULL_CAP) + codes % FULL_CAP
            places += jnp.arange(req_count)[:, None] * FULL_CAP
            chunk, stored = prepare()
            none = jnp.zeros((n_pref + LIST_PAD,), jnp.int32)
            acc, stats = attend_shared(none, *chunk, blocks)
            lists = listing(places, jnp.ones_like(places, dtype=bool))
            return attend_window(0, req_count, lists, chunk[0], acc, stats, blocks, None), *stored

        attn, k_out, v_out = lax.cond(fits, fast, full)
        return attn.reshape(queries.shape), k_out.reshape(k_pool.shape), v_out.reshape(v_pool.shape)

    row_spec = P('pool')
    return jax.shard_map(local_step, mesh=mesh, in_specs=(row_spec, row_spec, row_spec, row_spec, row_spec, P(), row_spec), out_specs=(row_spec, row_spec, row_spec), check_vma=False)
```
